32 devices in a mesh: bits: 16 (over z, y, x), docs: 2 (over core).
Axes of the slice: x: 2, y: 2, z: 4, core: 2. Of those that a mesh axis runs over, the one named last changes fastest.
Arguments:
- positions: int32 [1024, 4096], P(('bits', 'docs')), may hold values from 0 to 4095
- element_weights: float32 [1024, 1024], P(('bits', 'docs')), may hold values from 0.25 to 4
- set_sizes: int32 [1024], P(('bits', 'docs')), may hold values from 256 to 1024, as said below
- bit_weights: bfloat16 [4096], replicated, may hold values from 0.25 to 4
- candidates: int32 [2, 16, 16], P('docs'), may hold values from 0 to 63, as said below
Outputs:
- scores: float32 [2, 16, 128, 64], P('docs', 'bits')
The draws below stay inside these ranges and needn't reach their ends.
Inputs may be any that keep to these rules, and one draw needn't show every extreme that they name: `set_sizes`: one document in every draw has exactly 1024 elements. `candidates`: the 16 row tiles named for one block are distinct. `positions`: entries of a row beyond its first 4 * set_sizes are not part of the filter.
All inputs are finite; a program needn't handle non-finite values.
Results may differ from the reference program's by a relative error of at most 0.0012.
Values may be sent and summed in bfloat16 or wider, within the bound.
A program may use at most 64 MiB of HBM per device.

```python
import math
import jax
import jax.numpy as jnp
import numpy as np
from jax import lax

FILTER_BITS = 4096
HASHES = 4
ELEMS = 1024
TILE = 8
CAND = 16
PMAX = 4096
DOCS = 1024
ROW_GROUPS = 2
COL_BLOCKS = 16
ROW_HALF = 512
COLS = 64
RTILES = 64


def draw_set_sizes(key, part):
    levels = 64
    ladder = np.floor(ELEMS * 4.0 ** ((np.arange(levels) - (levels - 1)) / (levels - 1.0)))
    ladder = np.maximum(ladder, 1).astype(np.int32)
    pick_key, doc_key = jax.random.split(jax.random.fold_in(key, 11))
    picked = jax.random.randint(pick_key, (DOCS,), 0, levels)
    set_count = jnp.asarray(ladder)[picked]
    chosen_doc = jax.random.randint(doc_key, (), 0, DOCS)
    return set_count.at[chosen_doc].set(ELEMS).astype(jnp.int32)


def draw_candidates(key, part):
    block_keys = jax.random.split(jax.random.fold_in(key, 23), ROW_GROUPS * COL_BLOCKS)
    picked = jax.vmap(lambda sub_key: jax.random.permutation(sub_key, RTILES)[:CAND])(block_keys)
    return picked.reshape(ROW_GROUPS, COL_BLOCKS, CAND).astype(jnp.int32)


def place_ends(entries, stream_key, least, high):
    place = [jax.random.randint(jax.random.fold_in(stream_key, axis), (), 0, length) for axis, length in enumerate(entries.shape)]
    main_axis = entries.shape.index(max(entries.shape))
    beside = place[:main_axis] + [(place[main_axis] + 1) % entries.shape[main_axis]] + place[main_axis + 1:]
    return entries.at[tuple(place)].set(least).at[tuple(beside)].set(high)


def block_levels(rng, extent, pieces, least, top_value):
    factor_of = 1.0
    for dim, shards_of in pieces:
        steps = jax.random.uniform(jax.random.fold_in(jax.random.fold_in(rng, 6), dim), (shards_of,), jnp.float32, least / len(pieces), top_value / len(pieces))
        factor_of = factor_of * jnp.repeat(jnp.exp(steps), extent[dim] // shards_of).reshape((-1,) + (1,) * (len(extent) - 1 - dim))
    return factor_of


def setup_inputs(seed: int = 0) -> dict:
    key_of = jax.random.split(jax.random.key(seed), 6)
    positions = place_ends(jax.random.randint(key_of[0], (DOCS, PMAX), 0, FILTER_BITS), jax.random.fold_in(key_of[0], 1), 0, FILTER_BITS - 1).astype(jnp.int32)
    element_weights = jnp.clip(jnp.exp(math.log(4.0) - 2.7725887 * jax.random.uniform(key_of[1], (DOCS, ELEMS), jnp.float32) ** block_levels(key_of[1], (DOCS, ELEMS), ((0, 32),), -0.2, 0.2)), 0.25, 4.0)
    set_sizes = draw_set_sizes(jax.random.fold_in(key_of[5], 71), 0)
    bit_weights = jnp.clip(jnp.exp(jax.random.uniform(key_of[3], (FILTER_BITS,), jnp.float32, math.log(0.25), math.log(4.0))), 0.25, 4.0).astype(jnp.bfloat16)
    candidates = draw_candidates(jax.random.fold_in(key_of[5], 71), 0)
    return {"positions": positions, "element_weights": element_weights, "set_sizes": set_sizes, "bit_weights": bit_weights, "candidates": candidates}


def build_filter(positions, element_weights, set_sizes):
    doc_count, slot_count = positions.shape
    slot_index = jnp.arange(slot_count, dtype=jnp.int32)
    usable = slot_index[None, :] < HASHES * set_sizes[:, None]
    target = jnp.where(usable, positions, FILTER_BITS).astype(jnp.int32)
    row_index = jnp.broadcast_to(jnp.arange(doc_count, dtype=jnp.int32)[:, None], positions.shape)
    slot_weights = jnp.repeat(element_weights.astype(jnp.float32), HASHES, axis=1)
    summed = jnp.zeros((doc_count, FILTER_BITS), jnp.float32).at[row_index, target].add(slot_weights, mode="drop")
    return summed.astype(jnp.bfloat16)


def reference(positions, element_weights, set_sizes, bit_weights, candidates):
    cell_matrix = build_filter(positions, element_weights, set_sizes)
    weighted_all = cell_matrix * bit_weights
    popcount = jnp.sum(weighted_all.astype(jnp.float32) * cell_matrix.astype(jnp.float32), axis=1)
    offsets = jnp.arange(TILE, dtype=jnp.int32)
    starts = (jnp.arange(ROW_GROUPS, dtype=jnp.int32) * ROW_HALF)[:, None, None, None]
    row_docs = (starts + candidates[:, :, :, None] * TILE + offsets).reshape(ROW_GROUPS, COL_BLOCKS, CAND * TILE)
    row_docs = row_docs.astype(jnp.int32)
    columns = cell_matrix.reshape(COL_BLOCKS, COLS, FILTER_BITS).astype(jnp.float32)

    def one_group(group_rows):
        weighted = weighted_all[group_rows].astype(jnp.float32)
        return jnp.einsum("dcb,dkb->dck", weighted, columns, precision=lax.Precision.HIGHEST)

    shared = lax.map(one_group, row_docs)
    pop_rows = popcount[row_docs][..., None]
    pop_cols = popcount.reshape(COL_BLOCKS, COLS)[None, :, None, :]
    size_float = set_sizes.astype(jnp.float32)
    size_rows = size_float[row_docs][..., None]
    size_cols = size_float.reshape(COL_BLOCKS, COLS)[None, :, None, :]
    ratio = shared / (pop_rows + pop_cols - shared)
    return ratio * (size_rows + size_cols) / ((1.0 + ratio) * jnp.minimum(size_rows, size_cols))
```

```python
import functools
import math

import jax
import jax.numpy as jnp
from jax import lax
from jax.experimental import pallas as pl
from jax.experimental.pallas import tpu as pltpu
from jax.sharding import PartitionSpec as P

FILTER_BITS = 4096
HASHES = 4
TILE = 8
LANES = 128
CHUNK = 512
UNROLL = 4
PARTS = 2
MESH = pl.DeviceIdType.MESH


def build_filter(positions, element_weights, set_sizes):
    doc_count, slot_count = positions.shape
    elem_count = element_weights.shape[1]
    low_cells = 64
    high_cells = FILTER_BITS // low_cells
    slot_index = jnp.arange(slot_count, dtype=jnp.int32)
    usable = slot_index[None, :] < HASHES * set_sizes[:, None]
    spread = jnp.broadcast_to(element_weights[:, :, None], (doc_count, elem_count, HASHES)).reshape(
        doc_count, slot_count
    )
    slot_weights = jnp.where(usable, spread, 0.0)
    upper = slot_weights.astype(jnp.bfloat16)
    remain = slot_weights - upper.astype(jnp.float32)
    middle = remain.astype(jnp.bfloat16)
    lower = (remain - middle.astype(jnp.float32)).astype(jnp.bfloat16)
    weight_parts = jnp.stack([upper, middle, lower], axis=1)
    high_index = positions // low_cells
    low_index = positions - high_index * low_cells
    group = math.gcd(doc_count, 8)

    def one_group(inputs):
        part_block, high_block, low_block = inputs
        high_onehot = (high_block[:, :, None] == jnp.arange(high_cells, dtype=jnp.int32)).astype(
            jnp.bfloat16
        )
        low_onehot = (low_block[:, :, None] == jnp.arange(low_cells, dtype=jnp.int32)).astype(
            jnp.bfloat16
        )
        left = part_block[:, :, :, None] * high_onehot[:, None, :, :]
        summed = jnp.einsum("dcph,dpl->dhl", left, low_onehot, preferred_element_type=jnp.float32)
        return summed.reshape(group, FILTER_BITS)

    grouped = lax.map(
        one_group,
        (
            weight_parts.reshape(doc_count // group, group, 3, slot_count),
            high_index.reshape(doc_count // group, group, slot_count),
            low_index.reshape(doc_count // group, group, slot_count),
        ),
    )
    return grouped.reshape(doc_count, FILTER_BITS).astype(jnp.bfloat16)


def weighted_pop(cells, weights):
    weighted = cells * weights
    return jnp.sum(weighted.astype(jnp.float32) * cells.astype(jnp.float32), axis=1)


def estimate(shared, pop_rows, pop_cols, size_rows, size_cols):
    union_weight = pop_rows[:, None] + pop_cols[None, :] - shared
    ratio = shared / union_weight
    smaller = jnp.minimum(size_rows[:, None], size_cols[None, :])
    return ratio * (size_rows[:, None] + size_cols[None, :]) / ((1.0 + ratio) * smaller)


def pick_tiles(slice_cells, tile_choice, row_group, groups, row_half):
    width = slice_cells.shape[1]
    row_tiles = row_half // TILE
    tiles = slice_cells.reshape(groups, row_tiles, TILE * width)
    own_tiles = lax.dynamic_index_in_dim(tiles, row_group, 0, keepdims=False)
    onehot = (tile_choice[:, :, None] == jnp.arange(row_tiles, dtype=jnp.int32)).astype(
        jnp.bfloat16
    )
    picked = jnp.einsum("jcr,rw->jcw", onehot, own_tiles, preferred_element_type=jnp.float32)
    return picked.astype(jnp.bfloat16).reshape(
        tile_choice.shape[0], tile_choice.shape[1] * TILE, width
    )


def body(positions, element_weights, set_sizes, bit_weights, candidates):
    col_index = lax.axis_index("bits")
    row_group = lax.axis_index("docs")
    blocks = lax.axis_size("bits")
    groups = lax.axis_size("docs")
    doc_total = positions.shape[0] * blocks * groups
    row_half = doc_total // groups
    col_width = doc_total // blocks
    slot_count = candidates.shape[2] * TILE
    tile_offsets = jnp.arange(TILE, dtype=jnp.int32)
    own_cells = build_filter(positions, element_weights, set_sizes)
    local_pop = weighted_pop(own_cells, bit_weights)
    every_pop, size_float = (
        lax.all_gather(local_pop, ("bits", "docs"), axis=0, tiled=True),
        lax.all_gather(set_sizes.astype(jnp.float32), ("bits", "docs"), axis=0, tiled=True),
    )
    pair_cells = lax.all_gather(own_cells, "docs", axis=0, tiled=True)
    slice_cells = lax.all_to_all(pair_cells, "bits", split_axis=1, concat_axis=0, tiled=True)
    tile_rows = row_group * row_half + (candidates[0][:, :, None] * TILE + tile_offsets).reshape(
        blocks, slot_count
    )
    picked_cells = pick_tiles(slice_cells, candidates[0], row_group, groups, row_half)
    row_cells = lax.all_to_all(picked_cells, "bits", split_axis=0, concat_axis=2, tiled=True)[0]
    shared = lax.dot_general(
        row_cells * bit_weights,
        pair_cells,
        (((1,), (1,)), ((), ())),
        preferred_element_type=jnp.float32,
    )
    row_docs = lax.dynamic_index_in_dim(tile_rows, col_index, 0, keepdims=False)
    pop_rows = every_pop[row_docs]
    pop_cols = lax.dynamic_slice_in_dim(every_pop, col_index * col_width, col_width, 0)
    size_rows = size_float[row_docs]
    size_cols = lax.dynamic_slice_in_dim(size_float, col_index * col_width, col_width, 0)
    scores = estimate(shared, pop_rows, pop_cols, size_rows, size_cols)
    return scores.reshape(1, 1, slot_count, col_width)


NT = (((1,), (1,)), ((), ()))


def filter_kernel(sizes_ref, pos_ref, elem_ref, bw_ref, cells_ref, stats_ref, spread, acc, rows):
    docs, slots = pos_ref.shape
    elems = elem_ref.shape[1]
    highs = FILTER_BITS // LANES
    lane = lax.broadcasted_iota(jnp.int32, (docs, LANES), 1)
    sub = lax.broadcasted_iota(jnp.int32, (docs, LANES), 0)
    size_of = jnp.zeros((docs, LANES), jnp.int32)
    total = jnp.int32(0)
    for d in range(docs):
        size = sizes_ref[d]
        size_of = jnp.where(sub == d, size, size_of)
        total = total + (HASHES * size + CHUNK - 1) // CHUNK
    width = 2 * LANES
    wide = (lax.broadcasted_iota(jnp.int32, (width, HASHES * width), 1) // HASHES
            == lax.broadcasted_iota(jnp.int32, (width, HASHES * width), 0))
    wide = jnp.where(wide, 1.0, 0.0).astype(jnp.bfloat16)
    size_wide = jnp.concatenate([size_of] * (width // LANES), axis=1)
    lane_wide = lax.broadcasted_iota(jnp.int32, (docs, width), 1)
    for q in range(elems // width):
        value = elem_ref[:, q * width:(q + 1) * width]
        value = jnp.where(lane_wide + q * width < size_wide, value, 0.0)
        upper = value.astype(jnp.bfloat16)
        lower = (value - upper.astype(jnp.float32)).astype(jnp.bfloat16)
        for p, part in enumerate((upper, lower)):
            spread[p, :, q * HASHES * width:(q + 1) * HASHES * width] = jnp.dot(
                part, wide, preferred_element_type=jnp.float32)

    @pl.loop(0, docs + 1)
    def _(d):
        acc[d] = jnp.zeros(acc.shape[1:], jnp.float32)

    low_iota = lax.broadcasted_iota(jnp.int32, (LANES, CHUNK), 0)
    high_iota = lax.broadcasted_iota(jnp.int32, (highs, CHUNK), 0)

    def group(_, carry):
        d, c = carry
        for _ in range(UNROLL):
            row = jnp.minimum(d, docs - 1)
            at = pl.ds(pl.multiple_of(c * CHUNK, CHUNK), CHUNK)
            pos = pos_ref[pl.ds(row, 1), at]
            high, low = lax.shift_right_logical(pos, 7), lax.bitwise_and(pos, LANES - 1)
            left = jnp.where(low == low_iota, 1.0, 0.0).astype(jnp.bfloat16)
            hit = high == high_iota
            right = jnp.concatenate(
                [jnp.where(hit, spread[p, pl.ds(row, 1), at], 0.0) for p in range(PARTS)],
                axis=0).astype(jnp.bfloat16)
            acc[d] = acc[d] + lax.dot_general(left, right, NT, preferred_element_type=jnp.float32)
            more = (c + 1) * CHUNK < HASHES * sizes_ref[row]
            c = jnp.where(more, c + 1, 0)
            d = jnp.where(more, d, jnp.minimum(d + 1, docs))
            c = jnp.where(d == docs, 0, c)
        return d, c

    lax.fori_loop(0, (total + UNROLL - 1) // UNROLL, group, (jnp.int32(0), jnp.int32(0)))

    @pl.loop(0, docs)
    def _(d):
        both = acc[d].T
        rows[pl.ds(d, highs, stride=docs), :] = both[:highs] + both[highs:]

    span = cells_ref.shape[2]
    pop = jnp.zeros((docs, LANES), jnp.float32)
    for h in range(highs):
        cells = rows[h * docs:(h + 1) * docs, :].astype(jnp.bfloat16)
        cells_ref[h * LANES // span, :, h * LANES % span:h * LANES % span + LANES] = cells
        full = cells.astype(jnp.float32)
        weight = bw_ref[:, h * LANES:(h + 1) * LANES].astype(jnp.float32)
        pop = pop + (full * weight).astype(jnp.bfloat16).astype(jnp.float32) * full
    pop = jnp.sum(pop, axis=1, keepdims=True)
    both = jnp.where(lane == sub, pop, 0.0)
    both = jnp.where(lane == sub + docs, size_of.astype(jnp.float32), both)
    stats_ref[...] = jnp.sum(both, axis=0, keepdims=True)


def make_filter(positions, element_weights, set_sizes, weights, pieces):
    docs, slots = positions.shape
    vmem = pl.BlockSpec(memory_space=pltpu.VMEM)
    highs = FILTER_BITS // LANES
    return pl.pallas_call(
        filter_kernel,
        out_shape=(
            jax.ShapeDtypeStruct((pieces, docs, FILTER_BITS // pieces), jnp.bfloat16),
            jax.ShapeDtypeStruct((1, LANES), jnp.float32),
        ),
        in_specs=[pl.BlockSpec(memory_space=pltpu.SMEM), vmem, vmem, vmem],
        out_specs=(vmem, vmem),
        scratch_shapes=[
            pltpu.VMEM((PARTS, docs, slots), jnp.float32),
            pltpu.VMEM((docs + 1, LANES, PARTS * highs), jnp.float32),
            pltpu.VMEM((highs * docs, LANES), jnp.float32),
        ],
    )(set_sizes, positions, element_weights, weights)


def score_kernel(blocks, groups, cand_ref, cells_ref, stats_ref, bw_ref, out_ref,
                 slab, stat, weighted, part, inbox,
                 send1, recv1, send1s, recv1s, send2, recv2, send2s, recv2s, send3, recv3):
    col, grp = lax.axis_index("bits"), lax.axis_index("docs")
    docs, span = cells_ref.shape[1:]
    picks = cand_ref.shape[2]
    owners = blocks * groups
    row_half = docs * owners // groups
    width = docs * groups
    me = col * groups + grp

    barrier = pltpu.get_barrier_semaphore()
    for k in range(1, blocks):
        pl.semaphore_signal(barrier, inc=1, device_id=(lax.rem(col + k, blocks), grp), device_id_type=MESH)
    for k in range(1, groups):
        pl.semaphore_signal(barrier, inc=1, device_id=(col, lax.rem(grp + k, groups)), device_id_type=MESH)
    pl.semaphore_wait(barrier, blocks + groups - 2)

    def remote(src, dst, send, recv, device):
        return pltpu.make_async_remote_copy(
            src_ref=src, dst_ref=dst, send_sem=send, recv_sem=recv, device_id=device, device_id_type=MESH)

    first = []
    for k in range(1, blocks):
        to = lax.rem(col + k, blocks)
        first.append(remote(cells_ref.at[to], slab.at[me], send1.at[k], recv1.at[k], (to, grp)))
        first.append(remote(stats_ref.at[0], stat.at[me], send1s.at[k], recv1s.at[k], (to, grp)))
    for copy in first:
        copy.start()
    slab[me] = cells_ref[col]
    stat[me] = stats_ref[0]

    second = []
    other = lax.rem(grp + 1, groups)
    for k in range(blocks):
        if k:
            first[2 * k - 2].wait_recv()
            first[2 * k - 1].wait_recv()
        came = lax.rem(col - k + blocks, blocks)
        slot = came * groups + grp
        source = cells_ref.at[col] if k == 0 else slab.at[slot]
        source_s = stats_ref.at[0] if k == 0 else stat.at[slot]
        pair = (remote(source, slab.at[slot], send2.at[k], recv2.at[k], (col, other)),
                remote(source_s, stat.at[slot], send2s.at[k], recv2s.at[k], (col, other)))
        for copy in pair:
            copy.start()
        second.extend(pair)
    for copy in second:
        copy.wait_recv()

    bw = bw_ref[:, pl.ds(pl.multiple_of(col * span, span), span)].astype(jnp.float32)
    near = docs // TILE
    for o in range(owners // groups):
        value = slab[grp * (owners // groups) + o].astype(jnp.float32) * bw
        value = value.astype(jnp.bfloat16).astype(jnp.float32)
        for t in range(near):
            weighted[o * near + t] = value[t * TILE:(t + 1) * TILE]

    third = []
    for k in list(range(1, blocks)) + [0]:
        block = lax.rem(col + k, blocks)
        tiles = [weighted[cand_ref[0, block, c]] for c in range(picks)]
        lines = jnp.concatenate(tiles, axis=0).astype(jnp.bfloat16)
        columns = jnp.concatenate([slab[block * groups + o] for o in range(groups)], axis=0)
        part[k] = lax.dot_general(columns, lines, NT, preferred_element_type=jnp.float32)
        if k:
            copy = remote(part.at[k], inbox.at[k], send3.at[k], recv3.at[k], (block, grp))
            copy.start()
            third.append(copy)

    eight = lax.broadcasted_iota(jnp.int32, (TILE, LANES), 0)
    lanes = lax.broadcasted_iota(jnp.int32, (TILE, LANES), 1)
    pop_rows = jnp.zeros((TILE, LANES), jnp.float32)
    size_rows = jnp.zeros((TILE, LANES), jnp.float32)
    for c in range(picks):
        tile = cand_ref[0, col, c]
        line = stat[grp * (owners // groups) + lax.div(tile, near)]
        spot = lanes - lax.rem(tile, near) * TILE - eight
        pop = jnp.sum(jnp.where(spot == 0, line, 0.0), axis=1, keepdims=True)
        size = jnp.sum(jnp.where(spot == docs, line, 0.0), axis=1, keepdims=True)
        here = lanes == eight + c * TILE
        pop_rows = jnp.where(here, pop, pop_rows)
        size_rows = jnp.where(here, size, size_rows)
    pop_rows = jnp.sum(pop_rows, axis=0, keepdims=True)
    size_rows = jnp.sum(size_rows, axis=0, keepdims=True)
    sub = lax.broadcasted_iota(jnp.int32, (docs, LANES), 0)
    lane = lax.broadcasted_iota(jnp.int32, (docs, LANES), 1)
    mine = [stat[col * groups + o] for o in range(groups)]
    pop_cols = jnp.concatenate(
        [jnp.sum(jnp.where(lane == sub, line, 0.0), axis=1, keepdims=True) for line in mine], axis=0)
    size_cols = jnp.concatenate(
        [jnp.sum(jnp.where(lane == sub + docs, line, 0.0), axis=1, keepdims=True) for line in mine], axis=0)

    shared = part[0]
    for k, copy in enumerate(third):
        copy.wait_recv()
        shared = shared + inbox[k + 1]
    ratio = shared / (pop_rows + pop_cols - shared)
    out_ref[...] = ratio * (size_rows + size_cols) / ((1.0 + ratio) * jnp.minimum(size_rows, size_cols))
    for copy in first + second + third:
        copy.wait_send()


def fast_body(blocks, groups, positions, element_weights, set_sizes, bit_weights, candidates):
    docs = positions.shape[0]
    weights = bit_weights.reshape(1, -1)
    cells, stats = make_filter(positions, element_weights, set_sizes, weights, blocks)
    span = cells.shape[2]
    width, rows = docs * groups, candidates.shape[2] * TILE
    vmem = pl.BlockSpec(memory_space=pltpu.VMEM)
    sems = lambda: pltpu.SemaphoreType.DMA((blocks,))
    scores = pl.pallas_call(
        functools.partial(score_kernel, blocks, groups),
        out_shape=jax.ShapeDtypeStruct((width, rows), jnp.float32),
        in_specs=[pl.BlockSpec(memory_space=pltpu.SMEM), vmem, vmem, vmem],
        out_specs=vmem,
        scratch_shapes=[
            pltpu.VMEM((blocks * groups, docs, span), jnp.bfloat16),
            pltpu.VMEM((blocks * groups, 1, LANES), jnp.float32),
            pltpu.VMEM((docs * blocks // TILE, TILE, span), jnp.float32),
            pltpu.VMEM((blocks, width, rows), jnp.float32),
            pltpu.VMEM((blocks, width, rows), jnp.float32),
        ] + [sems() for _ in range(10)],
        compiler_params=pltpu.CompilerParams(collective_id=0, has_side_effects=True),
    )(candidates, cells, stats.reshape(1, 1, LANES), weights)
    return scores.T.reshape(1, 1, rows, width)


def solution(mesh):
    blocks, groups = mesh.shape["bits"], mesh.shape["docs"]
    fits = groups == 2 and FILTER_BITS % (blocks * LANES) == 0
    chosen = functools.partial(fast_body, blocks, groups) if fits else body
    return jax.shard_map(
        chosen,
        mesh=mesh,
        in_specs=(
            P(("bits", "docs"), None),
            P(("bits", "docs"), None),
            P(("bits", "docs")),
            P(),
            P("docs", None, None),
        ),
        out_specs=P("docs", "bits", None, None),
        check_vma=False,
    )
```

```python
import functools
import math

import jax
import jax.numpy as jnp
from jax import lax
from jax.experimental import pallas as pl
from jax.experimental.pallas import tpu as pltpu
from jax.sharding import PartitionSpec as P

FILTER_BITS = 4096
HASHES = 4
TILE = 8
LANES = 128
CHUNK = 512
UNROLL = 12
PARTS = 2
MESH = pl.DeviceIdType.MESH


def build_filter(positions, element_weights, set_sizes):
    doc_count, slot_count = positions.shape
    elem_count = element_weights.shape[1]
    low_cells = 64
    high_cells = FILTER_BITS // low_cells
    slot_index = jnp.arange(slot_count, dtype=jnp.int32)
    usable = slot_index[None, :] < HASHES * set_sizes[:, None]
    spread = jnp.broadcast_to(element_weights[:, :, None], (doc_count, elem_count, HASHES)).reshape(
        doc_count, slot_count
    )
    slot_weights = jnp.where(usable, spread, 0.0)
    upper = slot_weights.astype(jnp.bfloat16)
    remain = slot_weights - upper.astype(jnp.float32)
    middle = remain.astype(jnp.bfloat16)
    lower = (remain - middle.astype(jnp.float32)).astype(jnp.bfloat16)
    weight_parts = jnp.stack([upper, middle, lower], axis=1)
    high_index = positions // low_cells
    low_index = positions - high_index * low_cells
    group = math.gcd(doc_count, 8)

    def one_group(inputs):
        part_block, high_block, low_block = inputs
        high_onehot = (high_block[:, :, None] == jnp.arange(high_cells, dtype=jnp.int32)).astype(
            jnp.bfloat16
        )
        low_onehot = (low_block[:, :, None] == jnp.arange(low_cells, dtype=jnp.int32)).astype(
            jnp.bfloat16
        )
        left = part_block[:, :, :, None] * high_onehot[:, None, :, :]
        summed = jnp.einsum("dcph,dpl->dhl", left, low_onehot, preferred_element_type=jnp.float32)
        return summed.reshape(group, FILTER_BITS)

    grouped = lax.map(
        one_group,
        (
            weight_parts.reshape(doc_count // group, group, 3, slot_count),
            high_index.reshape(doc_count // group, group, slot_count),
            low_index.reshape(doc_count // group, group, slot_count),
        ),
    )
    return grouped.reshape(doc_count, FILTER_BITS).astype(jnp.bfloat16)


def weighted_pop(cells, weights):
    weighted = cells * weights
    return jnp.sum(weighted.astype(jnp.float32) * cells.astype(jnp.float32), axis=1)


def estimate(shared, pop_rows, pop_cols, size_rows, size_cols):
    union_weight = pop_rows[:, None] + pop_cols[None, :] - shared
    ratio = shared / union_weight
    smaller = jnp.minimum(size_rows[:, None], size_cols[None, :])
    return ratio * (size_rows[:, None] + size_cols[None, :]) / ((1.0 + ratio) * smaller)


def pick_tiles(slice_cells, tile_choice, row_group, groups, row_half):
    width = slice_cells.shape[1]
    row_tiles = row_half // TILE
    tiles = slice_cells.reshape(groups, row_tiles, TILE * width)
    own_tiles = lax.dynamic_index_in_dim(tiles, row_group, 0, keepdims=False)
    onehot = (tile_choice[:, :, None] == jnp.arange(row_tiles, dtype=jnp.int32)).astype(
        jnp.bfloat16
    )
    picked = jnp.einsum("jcr,rw->jcw", onehot, own_tiles, preferred_element_type=jnp.float32)
    return picked.astype(jnp.bfloat16).reshape(
        tile_choice.shape[0], tile_choice.shape[1] * TILE, width
    )


def body(positions, element_weights, set_sizes, bit_weights, candidates):
    col_index = lax.axis_index("bits")
    row_group = lax.axis_index("docs")
    blocks = lax.axis_size("bits")
    groups = lax.axis_size("docs")
    doc_total = positions.shape[0] * blocks * groups
    row_half = doc_total // groups
    col_width = doc_total // blocks
    slot_count = candidates.shape[2] * TILE
    tile_offsets = jnp.arange(TILE, dtype=jnp.int32)
    own_cells = build_filter(positions, element_weights, set_sizes)
    local_pop = weighted_pop(own_cells, bit_weights)
    every_pop, size_float = (
        lax.all_gather(local_pop, ("bits", "docs"), axis=0, tiled=True),
        lax.all_gather(set_sizes.astype(jnp.float32), ("bits", "docs"), axis=0, tiled=True),
    )
    pair_cells = lax.all_gather(own_cells, "docs", axis=0, tiled=True)
    slice_cells = lax.all_to_all(pair_cells, "bits", split_axis=1, concat_axis=0, tiled=True)
    tile_rows = row_group * row_half + (candidates[0][:, :, None] * TILE + tile_offsets).reshape(
        blocks, slot_count
    )
    picked_cells = pick_tiles(slice_cells, candidates[0], row_group, groups, row_half)
    row_cells = lax.all_to_all(picked_cells, "bits", split_axis=0, concat_axis=2, tiled=True)[0]
    shared = lax.dot_general(
        row_cells * bit_weights,
        pair_cells,
        (((1,), (1,)), ((), ())),
        preferred_element_type=jnp.float32,
    )
    row_docs = lax.dynamic_index_in_dim(tile_rows, col_index, 0, keepdims=False)
    pop_rows = every_pop[row_docs]
    pop_cols = lax.dynamic_slice_in_dim(every_pop, col_index * col_width, col_width, 0)
    size_rows = size_float[row_docs]
    size_cols = lax.dynamic_slice_in_dim(size_float, col_index * col_width, col_width, 0)
    scores = estimate(shared, pop_rows, pop_cols, size_rows, size_cols)
    return scores.reshape(1, 1, slot_count, col_width)


NT = (((1,), (1,)), ((), ()))


def filter_kernel(sizes_ref, pos_ref, elem_ref, bw_ref, cells_ref, stats_ref, spread, acc, rows):
    docs, slots = pos_ref.shape
    elems = elem_ref.shape[1]
    highs = FILTER_BITS // LANES
    lane = lax.broadcasted_iota(jnp.int32, (docs, LANES), 1)
    sub = lax.broadcasted_iota(jnp.int32, (docs, LANES), 0)
    size_of = jnp.zeros((docs, LANES), jnp.int32)
    total = jnp.int32(0)
    for d in range(docs):
        size = sizes_ref[d]
        size_of = jnp.where(sub == d, size, size_of)
        total = total + (HASHES * size + CHUNK - 1) // CHUNK
    width = 2 * LANES
    wide = (lax.broadcasted_iota(jnp.int32, (width, HASHES * width), 1) // HASHES
            == lax.broadcasted_iota(jnp.int32, (width, HASHES * width), 0))
    wide = jnp.where(wide, 1.0, 0.0).astype(jnp.bfloat16)
    size_wide = jnp.concatenate([size_of] * (width // LANES), axis=1)
    lane_wide = lax.broadcasted_iota(jnp.int32, (docs, width), 1)
    for q in range(elems // width):
        value = elem_ref[:, q * width:(q + 1) * width]
        value = jnp.where(lane_wide + q * width < size_wide, value, 0.0)
        upper = value.astype(jnp.bfloat16)
        lower = (value - upper.astype(jnp.float32)).astype(jnp.bfloat16)
        for p, part in enumerate((upper, lower)):
            spread[p, :, q * HASHES * width:(q + 1) * HASHES * width] = jnp.dot(
                part, wide, preferred_element_type=jnp.float32)

    @pl.loop(0, docs + 1)
    def _(d):
        acc[d] = jnp.zeros(acc.shape[1:], jnp.float32)

    low_iota = lax.broadcasted_iota(jnp.int32, (LANES, CHUNK), 0)
    high_iota = lax.broadcasted_iota(jnp.int32, (highs, CHUNK), 0)

    def group(_, carry):
        d, c = carry
        for _ in range(UNROLL):
            row = jnp.minimum(d, docs - 1)
            at = pl.ds(pl.multiple_of(c * CHUNK, CHUNK), CHUNK)
            pos = pos_ref[pl.ds(row, 1), at]
            high, low = lax.shift_right_logical(pos, 7), lax.bitwise_and(pos, LANES - 1)
            left = jnp.where(low == low_iota, 1.0, 0.0).astype(jnp.bfloat16)
            hit = high == high_iota
            right = jnp.concatenate(
                [jnp.where(hit, spread[p, pl.ds(row, 1), at], 0.0) for p in range(PARTS)],
                axis=0).astype(jnp.bfloat16)
            acc[d] = acc[d] + lax.dot_general(left, right, NT, preferred_element_type=jnp.float32)
            more = (c + 1) * CHUNK < HASHES * sizes_ref[row]
            c = jnp.where(more, c + 1, 0)
            d = jnp.where(more, d, jnp.minimum(d + 1, docs))
            c = jnp.where(d == docs, 0, c)
        return d, c

    lax.fori_loop(0, (total + UNROLL - 1) // UNROLL, group, (jnp.int32(0), jnp.int32(0)))

    @pl.loop(0, docs)
    def _(d):
        both = acc[d].T
        rows[pl.ds(d, highs, stride=docs), :] = both[:highs] + both[highs:]

    span = cells_ref.shape[2]
    pop = jnp.zeros((docs, LANES), jnp.float32)
    for h in range(highs):
        cells = rows[h * docs:(h + 1) * docs, :].astype(jnp.bfloat16)
        cells_ref[h * LANES // span, :, h * LANES % span:h * LANES % span + LANES] = cells
        full = cells.astype(jnp.float32)
        weight = bw_ref[h * LANES:(h + 1) * LANES].astype(jnp.float32).reshape(1, LANES)
        pop = pop + (full * weight).astype(jnp.bfloat16).astype(jnp.float32) * full
    pop = jnp.sum(pop, axis=1, keepdims=True)
    both = jnp.where(lane == sub, pop, 0.0)
    both = jnp.where(lane == sub + docs, size_of.astype(jnp.float32), both)
    stats_ref[...] = jnp.sum(both, axis=0, keepdims=True)


def make_filter(positions, element_weights, set_sizes, weights, pieces):
    docs, slots = positions.shape
    vmem = pl.BlockSpec(memory_space=pltpu.VMEM)
    highs = FILTER_BITS // LANES
    return pl.pallas_call(
        filter_kernel,
        out_shape=(
            jax.ShapeDtypeStruct((pieces, docs, FILTER_BITS // pieces), jnp.bfloat16),
            jax.ShapeDtypeStruct((1, LANES), jnp.float32),
        ),
        in_specs=[pl.BlockSpec(memory_space=pltpu.SMEM), vmem, vmem, vmem],
        out_specs=(vmem, vmem),
        scratch_shapes=[
            pltpu.VMEM((PARTS, docs, slots), jnp.float32),
            pltpu.VMEM((docs + 1, LANES, PARTS * highs), jnp.float32),
            pltpu.VMEM((highs * docs, LANES), jnp.float32),
        ],
    )(set_sizes, positions, element_weights, weights)


def score_kernel(blocks, groups, cand_ref, cells_ref, stats_ref, bw_ref, out_ref,
                 slab, stat, weighted, part, inbox,
                 send1, recv1, send1s, recv1s, send2, recv2, send2s, recv2s, send3, recv3):
    col, grp = lax.axis_index("bits"), lax.axis_index("docs")
    docs, span = cells_ref.shape[1:]
    picks = cand_ref.shape[2]
    owners = blocks * groups
    row_half = docs * owners // groups
    width = docs * groups
    me = col * groups + grp

    barrier = pltpu.get_barrier_semaphore()
    for k in range(1, blocks):
        pl.semaphore_signal(barrier, inc=1, device_id=(lax.rem(col + k, blocks), grp), device_id_type=MESH)
    for k in range(1, groups):
        pl.semaphore_signal(barrier, inc=1, device_id=(col, lax.rem(grp + k, groups)), device_id_type=MESH)
    pl.semaphore_wait(barrier, blocks + groups - 2)

    def remote(src, dst, send, recv, device):
        return pltpu.make_async_remote_copy(
            src_ref=src, dst_ref=dst, send_sem=send, recv_sem=recv, device_id=device, device_id_type=MESH)

    order = sorted(range(1, blocks), key=lambda k: -min(k, blocks - k))
    first, stats = {}, {}
    for k in order:
        to = lax.rem(col + k, blocks)
        first[k] = remote(cells_ref.at[to], slab.at[me], send1.at[k], recv1.at[k], (to, grp))
        stats[k] = remote(stats_ref.at[0], stat.at[me], send1s.at[k], recv1s.at[k], (to, grp))
        first[k].start()
        stats[k].start()
    slab[me] = cells_ref[col]
    stat[me] = stats_ref[0]

    second = []
    other = lax.rem(grp + 1, groups)
    for k in [0] + order[::-1]:
        if k:
            first[k].wait_recv()
            stats[k].wait_recv()
        came = lax.rem(col - k + blocks, blocks)
        slot = came * groups + grp
        source = cells_ref.at[col] if k == 0 else slab.at[slot]
        source_s = stats_ref.at[0] if k == 0 else stat.at[slot]
        pair = (remote(source, slab.at[slot], send2.at[k], recv2.at[k], (col, other)),
                remote(source_s, stat.at[slot], send2s.at[k], recv2s.at[k], (col, other)))
        for copy in pair:
            copy.start()
        second.extend(pair)
    for copy in second:
        copy.wait_recv()

    bw = bw_ref[pl.ds(pl.multiple_of(col * span, span), span)].astype(jnp.float32).reshape(1, span)
    near = docs // TILE
    for o in range(owners // groups):
        value = slab[grp * (owners // groups) + o].astype(jnp.float32) * bw
        value = value.astype(jnp.bfloat16).astype(jnp.float32)
        for t in range(near):
            weighted[o * near + t] = value[t * TILE:(t + 1) * TILE]

    third = []
    for k in order + [0]:
        block = lax.rem(col + k, blocks)
        tiles = [weighted[cand_ref[0, block, c]] for c in range(picks)]
        lines = jnp.concatenate(tiles, axis=0).astype(jnp.bfloat16)
        columns = jnp.concatenate([slab[block * groups + o] for o in range(groups)], axis=0)
        shared = lax.dot_general(columns, lines, NT, preferred_element_type=jnp.float32)
        if k:
            part[k] = shared.astype(part.dtype)
            copy = remote(part.at[k], inbox.at[k], send3.at[k], recv3.at[k], (block, grp))
            copy.start()
            third.append((k, copy))

    eight = lax.broadcasted_iota(jnp.int32, (TILE, LANES), 0)
    lanes = lax.broadcasted_iota(jnp.int32, (TILE, LANES), 1)
    pop_rows = jnp.zeros((TILE, LANES), jnp.float32)
    size_rows = jnp.zeros((TILE, LANES), jnp.float32)
    for c in range(picks):
        tile = cand_ref[0, col, c]
        line = stat[grp * (owners // groups) + lax.div(tile, near)]
        spot = lanes - lax.rem(tile, near) * TILE - eight
        pop = jnp.sum(jnp.where(spot == 0, line, 0.0), axis=1, keepdims=True)
        size = jnp.sum(jnp.where(spot == docs, line, 0.0), axis=1, keepdims=True)
        here = lanes == eight + c * TILE
        pop_rows = jnp.where(here, pop, pop_rows)
        size_rows = jnp.where(here, size, size_rows)
    pop_rows = jnp.sum(pop_rows, axis=0, keepdims=True)
    size_rows = jnp.sum(size_rows, axis=0, keepdims=True)
    sub = lax.broadcasted_iota(jnp.int32, (docs, LANES), 0)
    lane = lax.broadcasted_iota(jnp.int32, (docs, LANES), 1)
    mine = [stat[col * groups + o] for o in range(groups)]
    pop_cols = jnp.concatenate(
        [jnp.sum(jnp.where(lane == sub, line, 0.0), axis=1, keepdims=True) for line in mine], axis=0)
    size_cols = jnp.concatenate(
        [jnp.sum(jnp.where(lane == sub + docs, line, 0.0), axis=1, keepdims=True) for line in mine], axis=0)

    for k, copy in third[::-1]:
        copy.wait_recv()
        shared = shared + inbox[k].astype(jnp.float32)
    ratio = shared / (pop_rows + pop_cols - shared)
    out_ref[...] = ratio * (size_rows + size_cols) / ((1.0 + ratio) * jnp.minimum(size_rows, size_cols))
    for copy in [*first.values(), *stats.values(), *second] + [copy for _, copy in third]:
        copy.wait_send()


def fast_body(blocks, groups, positions, element_weights, set_sizes, bit_weights, candidates):
    docs = positions.shape[0]
    weights = bit_weights
    cells, stats = make_filter(positions, element_weights, set_sizes, weights, blocks)
    span = cells.shape[2]
    width, rows = docs * groups, candidates.shape[2] * TILE
    vmem = pl.BlockSpec(memory_space=pltpu.VMEM)
    sems = lambda: pltpu.SemaphoreType.DMA((blocks,))
    scores = pl.pallas_call(
        functools.partial(score_kernel, blocks, groups),
        out_shape=jax.ShapeDtypeStruct((width, rows), jnp.float32),
        in_specs=[pl.BlockSpec(memory_space=pltpu.SMEM), vmem, vmem, vmem],
        out_specs=vmem,
        scratch_shapes=[
            pltpu.VMEM((blocks * groups, docs, span), jnp.bfloat16),
            pltpu.VMEM((blocks * groups, 1, LANES), jnp.float32),
            pltpu.VMEM((docs * blocks // TILE, TILE, span), jnp.float32),
            pltpu.VMEM((blocks, width, rows), jnp.bfloat16),
            pltpu.VMEM((blocks, width, rows), jnp.bfloat16),
        ] + [sems() for _ in range(10)],
        compiler_params=pltpu.CompilerParams(collective_id=0, has_side_effects=True),
    )(candidates, cells, stats.reshape(1, 1, LANES), weights)
    return scores.T.reshape(1, 1, rows, width)


def solution(mesh):
    blocks, groups = mesh.shape["bits"], mesh.shape["docs"]
    fits = groups == 2 and FILTER_BITS % (blocks * LANES) == 0
    chosen = functools.partial(fast_body, blocks, groups) if fits else body
    return jax.shard_map(
        chosen,
        mesh=mesh,
        in_specs=(
            P(("bits", "docs"), None),
            P(("bits", "docs"), None),
            P(("bits", "docs")),
            P(),
            P("docs", None, None),
        ),
        out_specs=P("docs", "bits", None, None),
        check_vma=False,
    )
```

```python
import functools
import math

import jax
import jax.numpy as jnp
from jax import lax
from jax.experimental import pallas as pl
from jax.experimental.pallas import tpu as pltpu
from jax.sharding import PartitionSpec as P

FILTER_BITS = 4096
HASHES = 4
TILE = 8
LANES = 128
CHUNK = 512
UNROLL = 12
PARTS = 2
NEAR = 2
MESH = pl.DeviceIdType.MESH


def build_filter(positions, element_weights, set_sizes):
    doc_count, slot_count = positions.shape
    elem_count = element_weights.shape[1]
    low_cells = 64
    high_cells = FILTER_BITS // low_cells
    slot_index = jnp.arange(slot_count, dtype=jnp.int32)
    usable = slot_index[None, :] < HASHES * set_sizes[:, None]
    spread = jnp.broadcast_to(element_weights[:, :, None], (doc_count, elem_count, HASHES)).reshape(
        doc_count, slot_count
    )
    slot_weights = jnp.where(usable, spread, 0.0)
    upper = slot_weights.astype(jnp.bfloat16)
    remain = slot_weights - upper.astype(jnp.float32)
    middle = remain.astype(jnp.bfloat16)
    lower = (remain - middle.astype(jnp.float32)).astype(jnp.bfloat16)
    weight_parts = jnp.stack([upper, middle, lower], axis=1)
    high_index = positions // low_cells
    low_index = positions - high_index * low_cells
    group = math.gcd(doc_count, 8)

    def one_group(inputs):
        part_block, high_block, low_block = inputs
        high_onehot = (high_block[:, :, None] == jnp.arange(high_cells, dtype=jnp.int32)).astype(
            jnp.bfloat16
        )
        low_onehot = (low_block[:, :, None] == jnp.arange(low_cells, dtype=jnp.int32)).astype(
            jnp.bfloat16
        )
        left = part_block[:, :, :, None] * high_onehot[:, None, :, :]
        summed = jnp.einsum("dcph,dpl->dhl", left, low_onehot, preferred_element_type=jnp.float32)
        return summed.reshape(group, FILTER_BITS)

    grouped = lax.map(
        one_group,
        (
            weight_parts.reshape(doc_count // group, group, 3, slot_count),
            high_index.reshape(doc_count // group, group, slot_count),
            low_index.reshape(doc_count // group, group, slot_count),
        ),
    )
    return grouped.reshape(doc_count, FILTER_BITS).astype(jnp.bfloat16)


def weighted_pop(cells, weights):
    weighted = cells * weights
    return jnp.sum(weighted.astype(jnp.float32) * cells.astype(jnp.float32), axis=1)


def estimate(shared, pop_rows, pop_cols, size_rows, size_cols):
    union_weight = pop_rows[:, None] + pop_cols[None, :] - shared
    ratio = shared / union_weight
    smaller = jnp.minimum(size_rows[:, None], size_cols[None, :])
    return ratio * (size_rows[:, None] + size_cols[None, :]) / ((1.0 + ratio) * smaller)


def pick_tiles(slice_cells, tile_choice, row_group, groups, row_half):
    width = slice_cells.shape[1]
    row_tiles = row_half // TILE
    tiles = slice_cells.reshape(groups, row_tiles, TILE * width)
    own_tiles = lax.dynamic_index_in_dim(tiles, row_group, 0, keepdims=False)
    onehot = (tile_choice[:, :, None] == jnp.arange(row_tiles, dtype=jnp.int32)).astype(
        jnp.bfloat16
    )
    picked = jnp.einsum("jcr,rw->jcw", onehot, own_tiles, preferred_element_type=jnp.float32)
    return picked.astype(jnp.bfloat16).reshape(
        tile_choice.shape[0], tile_choice.shape[1] * TILE, width
    )


def body(positions, element_weights, set_sizes, bit_weights, candidates):
    col_index = lax.axis_index("bits")
    row_group = lax.axis_index("docs")
    blocks = lax.axis_size("bits")
    groups = lax.axis_size("docs")
    doc_total = positions.shape[0] * blocks * groups
    row_half = doc_total // groups
    col_width = doc_total // blocks
    slot_count = candidates.shape[2] * TILE
    tile_offsets = jnp.arange(TILE, dtype=jnp.int32)
    own_cells = build_filter(positions, element_weights, set_sizes)
    local_pop = weighted_pop(own_cells, bit_weights)
    every_pop, size_float = (
        lax.all_gather(local_pop, ("bits", "docs"), axis=0, tiled=True),
        lax.all_gather(set_sizes.astype(jnp.float32), ("bits", "docs"), axis=0, tiled=True),
    )
    pair_cells = lax.all_gather(own_cells, "docs", axis=0, tiled=True)
    slice_cells = lax.all_to_all(pair_cells, "bits", split_axis=1, concat_axis=0, tiled=True)
    tile_rows = row_group * row_half + (candidates[0][:, :, None] * TILE + tile_offsets).reshape(
        blocks, slot_count
    )
    picked_cells = pick_tiles(slice_cells, candidates[0], row_group, groups, row_half)
    row_cells = lax.all_to_all(picked_cells, "bits", split_axis=0, concat_axis=2, tiled=True)[0]
    shared = lax.dot_general(
        row_cells * bit_weights,
        pair_cells,
        (((1,), (1,)), ((), ())),
        preferred_element_type=jnp.float32,
    )
    row_docs = lax.dynamic_index_in_dim(tile_rows, col_index, 0, keepdims=False)
    pop_rows = every_pop[row_docs]
    pop_cols = lax.dynamic_slice_in_dim(every_pop, col_index * col_width, col_width, 0)
    size_rows = size_float[row_docs]
    size_cols = lax.dynamic_slice_in_dim(size_float, col_index * col_width, col_width, 0)
    scores = estimate(shared, pop_rows, pop_cols, size_rows, size_cols)
    return scores.reshape(1, 1, slot_count, col_width)


NT = (((1,), (1,)), ((), ()))


def filter_kernel(sizes_ref, pos_ref, elem_ref, bw_ref, cells_ref, stats_ref, spread, acc, rows):
    docs, slots = pos_ref.shape
    elems = elem_ref.shape[1]
    highs = FILTER_BITS // LANES
    lane = lax.broadcasted_iota(jnp.int32, (docs, LANES), 1)
    sub = lax.broadcasted_iota(jnp.int32, (docs, LANES), 0)
    size_of = jnp.zeros((docs, LANES), jnp.int32)
    total = jnp.int32(0)
    for d in range(docs):
        size = sizes_ref[d]
        size_of = jnp.where(sub == d, size, size_of)
        total = total + (HASHES * size + CHUNK - 1) // CHUNK
    width = 2 * LANES
    wide = (lax.broadcasted_iota(jnp.int32, (width, HASHES * width), 1) // HASHES
            == lax.broadcasted_iota(jnp.int32, (width, HASHES * width), 0))
    wide = jnp.where(wide, 1.0, 0.0).astype(jnp.bfloat16)
    size_wide = jnp.concatenate([size_of] * (width // LANES), axis=1)
    lane_wide = lax.broadcasted_iota(jnp.int32, (docs, width), 1)
    for q in range(elems // width):
        value = elem_ref[:, q * width:(q + 1) * width]
        value = jnp.where(lane_wide + q * width < size_wide, value, 0.0)
        upper = value.astype(jnp.bfloat16)
        lower = (value - upper.astype(jnp.float32)).astype(jnp.bfloat16)
        for p, part in enumerate((upper, lower)):
            spread[p, :, q * HASHES * width:(q + 1) * HASHES * width] = jnp.dot(
                part, wide, preferred_element_type=jnp.float32)

    @pl.loop(0, docs + 1)
    def _(d):
        acc[d] = jnp.zeros(acc.shape[1:], jnp.float32)

    low_iota = lax.broadcasted_iota(jnp.int32, (LANES, CHUNK), 0)
    high_iota = lax.broadcasted_iota(jnp.int32, (highs, CHUNK), 0)

    def group(_, carry):
        d, c = carry
        for _ in range(UNROLL):
            row = jnp.minimum(d, docs - 1)
            at = pl.ds(pl.multiple_of(c * CHUNK, CHUNK), CHUNK)
            pos = pos_ref[pl.ds(row, 1), at]
            high, low = lax.shift_right_logical(pos, 7), lax.bitwise_and(pos, LANES - 1)
            left = jnp.where(low == low_iota, 1.0, 0.0).astype(jnp.bfloat16)
            hit = high == high_iota
            right = jnp.concatenate(
                [jnp.where(hit, spread[p, pl.ds(row, 1), at], 0.0) for p in range(PARTS)],
                axis=0).astype(jnp.bfloat16)
            acc[d] = acc[d] + lax.dot_general(left, right, NT, preferred_element_type=jnp.float32)
            more = (c + 1) * CHUNK < HASHES * sizes_ref[row]
            c = jnp.where(more, c + 1, 0)
            d = jnp.where(more, d, jnp.minimum(d + 1, docs))
            c = jnp.where(d == docs, 0, c)
        return d, c

    lax.fori_loop(0, (total + UNROLL - 1) // UNROLL, group, (jnp.int32(0), jnp.int32(0)))

    @pl.loop(0, docs)
    def _(d):
        both = acc[d].T
        rows[pl.ds(d, highs, stride=docs), :] = both[:highs] + both[highs:]

    span = cells_ref.shape[2]
    pop = jnp.zeros((docs, LANES), jnp.float32)
    for h in range(highs):
        cells = rows[h * docs:(h + 1) * docs, :].astype(jnp.bfloat16)
        cells_ref[h * LANES // span, :, h * LANES % span:h * LANES % span + LANES] = cells
        full = cells.astype(jnp.float32)
        weight = bw_ref[h * LANES:(h + 1) * LANES].astype(jnp.float32).reshape(1, LANES)
        pop = pop + (full * weight).astype(jnp.bfloat16).astype(jnp.float32) * full
    pop = jnp.sum(pop, axis=1, keepdims=True)
    both = jnp.where(lane == sub, pop, 0.0)
    both = jnp.where(lane == sub + docs, size_of.astype(jnp.float32), both)
    stats_ref[...] = jnp.sum(both, axis=0, keepdims=True)


def make_filter(positions, element_weights, set_sizes, weights, pieces):
    docs, slots = positions.shape
    vmem = pl.BlockSpec(memory_space=pltpu.VMEM)
    highs = FILTER_BITS // LANES
    return pl.pallas_call(
        filter_kernel,
        out_shape=(
            jax.ShapeDtypeStruct((pieces, docs, FILTER_BITS // pieces), jnp.bfloat16),
            jax.ShapeDtypeStruct((1, LANES), jnp.float32),
        ),
        in_specs=[pl.BlockSpec(memory_space=pltpu.SMEM), vmem, vmem, vmem],
        out_specs=(vmem, vmem),
        scratch_shapes=[
            pltpu.VMEM((PARTS, docs, slots), jnp.float32),
            pltpu.VMEM((docs + 1, LANES, PARTS * highs), jnp.float32),
            pltpu.VMEM((highs * docs, LANES), jnp.float32),
        ],
    )(set_sizes, positions, element_weights, weights)


def score_kernel(blocks, groups, cand_ref, cells_ref, stats_ref, bw_ref, out_ref,
                 slab, stat, weighted, part, inbox,
                 send1, recv1, send1s, recv1s, sendx, recvx, sendxs, recvxs, send2, recv2, send2s, recv2s,
                 send3, recv3):
    col, grp = lax.axis_index("bits"), lax.axis_index("docs")
    docs, span = cells_ref.shape[1:]
    picks = cand_ref.shape[2]
    owners = blocks * groups
    row_half = docs * owners // groups
    width = docs * groups
    me = col * groups + grp

    pieces = blocks // NEAR
    piece, side = lax.div(col, NEAR), lax.rem(col, NEAR)
    other = lax.rem(grp + 1, groups)
    across = piece * NEAR + (NEAR - 1 - side)

    barrier = pltpu.get_barrier_semaphore()
    for k in range(1, pieces):
        to = lax.rem(piece + k, pieces) * NEAR + side
        pl.semaphore_signal(barrier, inc=1, device_id=(to, grp), device_id_type=MESH)
    pl.semaphore_signal(barrier, inc=1, device_id=(across, grp), device_id_type=MESH)
    pl.semaphore_signal(barrier, inc=1, device_id=(col, other), device_id_type=MESH)
    pl.semaphore_wait(barrier, pieces + 1)

    def remote(src, dst, send, recv, device):
        return pltpu.make_async_remote_copy(
            src_ref=src, dst_ref=dst, send_sem=send, recv_sem=recv, device_id=device, device_id_type=MESH)

    order = sorted(range(1, pieces), key=lambda k: -min(k, pieces - k))
    copies, first = [], {}
    for k in order:
        to = lax.rem(piece + k, pieces)
        first[k] = (remote(cells_ref.at[to], slab.at[me], send1.at[k], recv1.at[k], (to * NEAR + side, grp)),
                    remote(stats_ref.at[0], stat.at[me], send1s.at[k], recv1s.at[k], (to * NEAR + side, grp)))
        for copy in first[k]:
            copy.start()
        copies.extend(first[k])
    slab[me] = cells_ref[piece]
    stat[me] = stats_ref[0]

    def to_pair(slot, source, source_s, k):
        pair = (remote(source, slab.at[slot], send2.at[k], recv2.at[k], (col, other)),
                remote(source_s, stat.at[slot], send2s.at[k], recv2s.at[k], (col, other)))
        for copy in pair:
            copy.start()
        copies.extend(pair)
        second.extend(pair)

    second, sides = [], {}
    for k in [0] + order[::-1]:
        if k:
            for copy in first[k]:
                copy.wait_recv()
        came = lax.rem(piece - k + pieces, pieces) * NEAR + side
        slot = came * groups + grp
        source = slab.at[slot] if k else cells_ref.at[piece]
        source_s = stat.at[slot] if k else stats_ref.at[0]
        sides[k] = (remote(source, slab.at[slot], sendx.at[k], recvx.at[k], (across, grp)),
                    remote(source_s, stat.at[slot], sendxs.at[k], recvxs.at[k], (across, grp)))
        for copy in sides[k]:
            copy.start()
        copies.extend(sides[k])
        to_pair(slot, source, source_s, k)
    for k in [0] + order[::-1]:
        for copy in sides[k]:
            copy.wait_recv()
        came = lax.rem(piece - k + pieces, pieces) * NEAR + (NEAR - 1 - side)
        slot = came * groups + grp
        to_pair(slot, slab.at[slot], stat.at[slot], pieces + k)
    for copy in second:
        copy.wait_recv()

    bw = bw_ref[pl.ds(pl.multiple_of(piece * span, span), span)].astype(jnp.float32).reshape(1, span)
    near = docs // TILE
    for o in range(owners // groups):
        value = slab[grp * (owners // groups) + o].astype(jnp.float32) * bw
        value = value.astype(jnp.bfloat16).astype(jnp.float32)
        for t in range(near):
            weighted[o * near + t] = value[t * TILE:(t + 1) * TILE]

    third = []
    for k in order + [0]:
        block = lax.rem(piece + k, pieces) * NEAR + side
        tiles = [weighted[cand_ref[0, block, c]] for c in range(picks)]
        lines = jnp.concatenate(tiles, axis=0).astype(jnp.bfloat16)
        columns = jnp.concatenate([slab[block * groups + o] for o in range(groups)], axis=0)
        shared = lax.dot_general(columns, lines, NT, preferred_element_type=jnp.float32)
        if k:
            part[k] = shared.astype(part.dtype)
            copy = remote(part.at[k], inbox.at[k], send3.at[k], recv3.at[k], (block, grp))
            copy.start()
            third.append((k, copy))

    eight = lax.broadcasted_iota(jnp.int32, (TILE, LANES), 0)
    lanes = lax.broadcasted_iota(jnp.int32, (TILE, LANES), 1)
    pop_rows = jnp.zeros((TILE, LANES), jnp.float32)
    size_rows = jnp.zeros((TILE, LANES), jnp.float32)
    for c in range(picks):
        tile = cand_ref[0, col, c]
        line = stat[grp * (owners // groups) + lax.div(tile, near)]
        spot = lanes - lax.rem(tile, near) * TILE - eight
        pop = jnp.sum(jnp.where(spot == 0, line, 0.0), axis=1, keepdims=True)
        size = jnp.sum(jnp.where(spot == docs, line, 0.0), axis=1, keepdims=True)
        here = lanes == eight + c * TILE
        pop_rows = jnp.where(here, pop, pop_rows)
        size_rows = jnp.where(here, size, size_rows)
    pop_rows = jnp.sum(pop_rows, axis=0, keepdims=True)
    size_rows = jnp.sum(size_rows, axis=0, keepdims=True)
    sub = lax.broadcasted_iota(jnp.int32, (docs, LANES), 0)
    lane = lax.broadcasted_iota(jnp.int32, (docs, LANES), 1)
    mine = [stat[col * groups + o] for o in range(groups)]
    pop_cols = jnp.concatenate(
        [jnp.sum(jnp.where(lane == sub, line, 0.0), axis=1, keepdims=True) for line in mine], axis=0)
    size_cols = jnp.concatenate(
        [jnp.sum(jnp.where(lane == sub + docs, line, 0.0), axis=1, keepdims=True) for line in mine], axis=0)

    for k, copy in third[::-1]:
        copy.wait_recv()
        shared = shared + inbox[k].astype(jnp.float32)
    ratio = shared / (pop_rows + pop_cols - shared)
    out_ref[...] = ratio * (size_rows + size_cols) / ((1.0 + ratio) * jnp.minimum(size_rows, size_cols))
    for copy in copies + [copy for _, copy in third]:
        copy.wait_send()


def fast_body(blocks, groups, positions, element_weights, set_sizes, bit_weights, candidates):
    docs = positions.shape[0]
    weights = bit_weights
    cells, stats = make_filter(positions, element_weights, set_sizes, weights, blocks // NEAR)
    span = cells.shape[2]
    width, rows = docs * groups, candidates.shape[2] * TILE
    vmem = pl.BlockSpec(memory_space=pltpu.VMEM)
    sems = lambda: pltpu.SemaphoreType.DMA((blocks,))
    scores = pl.pallas_call(
        functools.partial(score_kernel, blocks, groups),
        out_shape=jax.ShapeDtypeStruct((width, rows), jnp.float32),
        in_specs=[pl.BlockSpec(memory_space=pltpu.SMEM), vmem, vmem, vmem],
        out_specs=vmem,
        scratch_shapes=[
            pltpu.VMEM((blocks * groups, docs, span), jnp.bfloat16),
            pltpu.VMEM((blocks * groups, 1, LANES), jnp.float32),
            pltpu.VMEM((docs * blocks // TILE, TILE, span), jnp.float32),
            pltpu.VMEM((blocks // NEAR, width, rows), jnp.float32),
            pltpu.VMEM((blocks // NEAR, width, rows), jnp.float32),
        ] + [sems() for _ in range(14)],
        compiler_params=pltpu.CompilerParams(collective_id=0, has_side_effects=True),
    )(candidates, cells, stats.reshape(1, 1, LANES), weights)
    return scores.T.reshape(1, 1, rows, width)


def solution(mesh):
    blocks, groups = mesh.shape["bits"], mesh.shape["docs"]
    fits = groups == 2 and blocks % NEAR == 0 and FILTER_BITS % (blocks // NEAR * LANES) == 0
    chosen = functools.partial(fast_body, blocks, groups) if fits else body
    return jax.shard_map(
        chosen,
        mesh=mesh,
        in_specs=(
            P(("bits", "docs"), None),
            P(("bits", "docs"), None),
            P(("bits", "docs")),
            P(),
            P("docs", None, None),
        ),
        out_specs=P("docs", "bits", None, None),
        check_vma=False,
    )
```
